32 devices in a mesh: dp: 4 (over y, core), fsdp: 8 (over z, x).
Axes of the slice: x: 2, y: 2, z: 4, core: 2. Of those that a mesh axis runs over, the one named last changes fastest.
Arguments:
- data_samples: bfloat16 [512, 4096], P('dp', 'fsdp'), may hold values from -6 to 6
- negative_start: float32 [512, 4096], P('dp', 'fsdp'), may hold values from -6 to 6
- langevin_noise: float32 [4, 512, 4096], P(None, 'dp', 'fsdp'), may hold values from -6 to 6
- first_weight: bfloat16 [4096, 4096], P('fsdp'), may hold values from -0.09375 to 0.09375
- second_weight: bfloat16 [4096, 4096], P('fsdp'), may hold values from -0.09375 to 0.09375
- readout: float32 [4096], P('fsdp'), may hold values from -480 to 480
Outputs:
- first_grad: float32 [4096, 4096], P('fsdp', 'dp')
- second_grad: float32 [4096, 4096], P('fsdp', 'dp')
- energy_gap: float32 [], replicated
The draws below stay inside these ranges and needn't reach their ends.
All inputs are finite; a program needn't handle non-finite values.
Results may differ from the reference program's by a relative error of at most 0.014.
Values may be sent and summed in bfloat16 or wider, within the bound.
A program may use at most 64 MiB of HBM per device.

```python
import jax
import jax.numpy as jnp
from jax import lax

D = 4096
H = 4096
STEPS = 4
SAMPLES = 512
N_FSDP = 8


def levels(own_key, shape, cuts, least, high):
    level = 1.0
    for axis_at, shards_of in cuts:
        heights = jax.random.uniform(jax.random.fold_in(jax.random.fold_in(own_key, 6), axis_at), (shards_of,), jnp.float32, least / len(cuts), high / len(cuts))
        level = level * jnp.repeat(jnp.exp(heights), shape[axis_at] // shards_of).reshape((-1,) + (1,) * (len(shape) - 1 - axis_at))
    return level


def bell_draw(rng, extent, spread, most, cuts=(), kind=jnp.bfloat16):
    entries = jax.random.normal(rng, extent, jnp.float32) * spread
    if len(cuts) > 0:
        entries = levels(rng, extent, cuts, -0.22, 0.18) * entries
    return jnp.clip(entries, min=-most, max=most).astype(kind)


def setup_inputs(seed: int = 0) -> dict:
    arg_keys = jax.random.split(jax.random.key(seed), 7)
    return {
        "data_samples": bell_draw(arg_keys[0], (SAMPLES, D), 1.0, 6.0, ((0, 4), (1, 8))),
        "negative_start": bell_draw(arg_keys[1], (SAMPLES, D), 1.0, 6.0, ((0, 4), (1, 8)), jnp.float32),
        "langevin_noise": bell_draw(arg_keys[2], (STEPS, SAMPLES, D), 1.0, 6.0, ((1, 4), (2, 8)), jnp.float32),
        "first_weight": bell_draw(arg_keys[3], (D, H), D ** -0.5, 0.09375, ((0, 8),)),
        "second_weight": bell_draw(arg_keys[4], (H, H), H ** -0.5, 0.09375, ((0, 8),)),
        "readout": bell_draw(arg_keys[5], (H,), 80.0, 480.0, ((0, 8),), jnp.float32),
    }


def slope(values):
    sig = jax.nn.sigmoid(values)
    return sig * (1.0 + values * (1.0 - sig))

def layer(inputs, weight):
    count = inputs.shape[0]
    width = weight.shape[0]
    pieces = jnp.einsum('rnk,nkh->nrh', inputs.reshape(count, N_FSDP, width // N_FSDP).astype(jnp.float32), weight.reshape(N_FSDP, width // N_FSDP, weight.shape[1]).astype(jnp.float32), precision=lax.Precision.HIGHEST)
    rounded = lax.optimization_barrier(pieces.astype(jnp.bfloat16))
    return lax.optimization_barrier(jnp.sum(rounded.astype(jnp.float32), axis=0))

def forward(inputs, first_weight, second_weight):
    pre_one = layer(inputs, first_weight)
    hidden = jax.nn.silu(pre_one).astype(jnp.bfloat16)
    pre_two = layer(hidden, second_weight)
    return (pre_one, hidden, pre_two)

def backward(cotan, readout, pre_one, pre_two, second_weight):
    grad_two = (cotan[:, None] * readout[None, :] * slope(pre_two)).astype(jnp.bfloat16)
    back_one = jnp.dot(grad_two, second_weight.T, preferred_element_type=jnp.float32)
    grad_one = (back_one * slope(pre_one)).astype(jnp.bfloat16)
    return (grad_two, grad_one)

def reference(data_samples, negative_start, langevin_noise, first_weight, second_weight, readout):
    state = negative_start
    ones = jnp.ones((state.shape[0],), jnp.float32)
    for step in range(STEPS):
        inputs = state.astype(jnp.bfloat16)
        pre_one, hidden, pre_two = forward(inputs, first_weight, second_weight)
        grad_two, grad_one = backward(ones, readout, pre_one, pre_two, second_weight)
        moved = jnp.dot(grad_one, first_weight.T, preferred_element_type=jnp.float32)
        state = state - 0.005 * moved + 0.1 * langevin_noise[step]
    rows = jnp.concatenate([data_samples, state.astype(jnp.bfloat16)], axis=0)
    cotan = jnp.concatenate([ones, -ones])
    pre_one, hidden, pre_two = forward(rows, first_weight, second_weight)
    energies = jnp.dot(jax.nn.silu(pre_two), readout, precision=lax.Precision.HIGHEST)
    energy_gap = jnp.sum(cotan * energies) / (SAMPLES * 80.0 * jnp.sqrt(jnp.float32(H)))
    grad_two, grad_one = backward(cotan, readout, pre_one, pre_two, second_weight)
    raw_one = jnp.dot(rows.T, grad_one, preferred_element_type=jnp.float32)
    raw_two = jnp.dot(hidden.T, grad_two, preferred_element_type=jnp.float32)
    total = jnp.sum(raw_one * raw_one) + jnp.sum(raw_two * raw_two)
    scale = jnp.sqrt(total / (2.0 * D * H) + 1e-06)
    return (raw_one / scale, raw_two / scale, energy_gap)
```

```python
import functools

import jax
import jax.numpy as jnp
from jax import lax
from jax.experimental import pallas as pl
from jax.experimental.pallas import tpu as pltpu
from jax.sharding import PartitionSpec as P

MESH = pl.DeviceIdType.MESH
BF16 = jnp.bfloat16
F32 = jnp.float32


def inner_of(n):
    return max(i for i in range(1, n + 1) if n % i == 0 and i * i <= n)


def folded(values):
    rows, columns = values.shape
    tall = values.reshape(rows // 8, 8, columns).sum(axis=0)
    out = tall[:, :128]
    for at in range(128, columns, 128):
        out += tall[:, at : at + 128]
    return out


def kernel(
    n, X, dpn, steps,
    data_ref, start_ref, noise_ref, w1_ref, w2_ref, read_ref,
    raw1_ref, raw2_ref, stat_ref,
    state, s_a, r_a, s_b, r_b, acc, ag_data, ag_neg, rows_all, hid_all, g_all, own_stat, got_stat,
    sem_as, sem_ar, sem_bs, sem_br, sem_zs, sem_zr, sem_xs, sem_xr, sem_ds, sem_dr, sem_ts, sem_tr,
):
    Z = n // X
    q = n // dpn
    C = w1_ref.shape[1] // n
    me = lax.axis_index("fsdp")
    dpi = lax.axis_index("dp")
    z, x = me // X, me % X

    def dest(oz, ox):
        return ((z + oz) % Z) * X + (x + ox) % X

    def source(oz, ox):
        return ((z + Z - oz) % Z) * X + (x + X - ox) % X

    def dp_dest(o):
        return (dpi + o) % dpn

    def cols(at):
        return pl.ds(pl.multiple_of(at * C, C), C)

    def send(src, dst, ssem, rsem, axis, peer):
        return pltpu.make_async_remote_copy(
            src_ref=src, dst_ref=dst, send_sem=ssem, recv_sem=rsem,
            device_id={axis: peer}, device_id_type=MESH,
        )

    partners = (
        [("fsdp", dest(0, ox)) for ox in range(1, X)]
        + [("fsdp", dest(oz, 0)) for oz in range(1, Z)]
        + [("dp", dp_dest(o)) for o in range(1, dpn)]
    )
    barrier = pltpu.get_barrier_semaphore()
    for axis, peer in partners:
        pl.semaphore_signal(barrier, inc=1, device_id={axis: peer}, device_id_type=MESH)
    pl.semaphore_wait(barrier, len(partners))

    def settle(copies):
        for copy in copies:
            copy.wait_send()

    def reduce_scatter(j, lhs, w_ref):
        sent, from_x, from_z = [], {}, {}
        order = list(range(1, Z)) + [0]
        for oz in order:
            for ox in range(1, X):
                s_a[j, oz, ox - 1] = jnp.dot(
                    lhs, w_ref[:, cols(dest(oz, ox))], preferred_element_type=F32
                ).astype(BF16)
                copy = send(
                    s_a.at[j, oz, ox - 1], r_a.at[j, oz, ox - 1],
                    sem_as.at[j, oz, ox - 1], sem_ar.at[j, oz, ox - 1], "fsdp", dest(0, ox),
                )
                copy.start()
                sent.append(copy)
                from_x[oz, ox] = copy
        for oz in order:
            acc[oz] = jnp.dot(lhs, w_ref[:, cols(dest(oz, 0))], preferred_element_type=F32)

        def joined(oz):
            total = acc[oz]
            for ox in range(1, X):
                from_x[oz, ox].wait_recv()
                total += r_a[j, oz, ox - 1].astype(F32)
            return total

        for oz in range(1, Z):
            s_b[j, oz - 1] = joined(oz).astype(BF16)
            copy = send(
                s_b.at[j, oz - 1], r_b.at[j, oz - 1],
                sem_bs.at[j, oz - 1], sem_br.at[j, oz - 1], "fsdp", dest(oz, 0),
            )
            copy.start()
            sent.append(copy)
            from_z[oz] = copy
        total = joined(0)
        for oz in range(1, Z):
            from_z[oz].wait_recv()
            total += r_b[j, oz - 1].astype(F32)
        return total, sent

    def gather_dot(j, buf, w_ref):
        sent = []

        def block(at):
            return lax.dot_general(
                buf[at], w_ref[:, cols(at)], (((1,), (1,)), ((), ())), preferred_element_type=F32
            )

        def push(at, ssem, rsem, peer):
            copy = send(buf.at[at], buf.at[at], ssem, rsem, "fsdp", peer)
            copy.start()
            sent.append(copy)

        def arrive(at, ssem, rsem):
            send(buf.at[at], buf.at[at], ssem, rsem, "fsdp", dest(1, 0)).wait_recv()

        for oz in range(1, Z):
            push(me, sem_zs.at[j, oz - 1], sem_zr.at[j, oz - 1], dest(oz, 0))
        for ox in range(1, X):
            push(me, sem_xs.at[j, 0, ox - 1], sem_xr.at[j, 0, ox - 1], dest(0, ox))
        total = block(me)
        for oz in range(1, Z):
            at = source(oz, 0)
            arrive(at, sem_zs.at[j, oz - 1], sem_zr.at[j, oz - 1])
            for ox in range(1, X):
                push(at, sem_xs.at[j, oz, ox - 1], sem_xr.at[j, oz, ox - 1], dest(0, ox))
            total += block(at)
        for oz in range(Z):
            for ox in range(1, X):
                at = source(oz, ox)
                arrive(at, sem_xs.at[j, oz, ox - 1], sem_xr.at[j, oz, ox - 1])
                total += block(at)
        return total, sent

    def slope(a):
        s = jax.nn.sigmoid(a)
        return s * (1.0 + a * (1.0 - s))

    def one_pass(u, sign, buf, keep):
        a1, sent_1 = reduce_scatter(0, u, w1_ref)
        s1 = jax.nn.sigmoid(a1)
        hidden = (a1 * s1).astype(BF16)
        slope_1 = s1 * (1.0 + a1 * (1.0 - s1))
        a2, sent_2 = reduce_scatter(1, hidden, w2_ref)
        settle(sent_1)
        g2 = (sign * read_ref[...] * slope(a2)).astype(BF16)
        buf[0, me] = g2
        back, sent_3 = gather_dot(0, buf.at[0], w2_ref)
        settle(sent_2)
        buf[1, me] = (back * slope_1).astype(BF16)
        waits = keep(0, u, hidden, a2)
        moved, sent_4 = gather_dot(1, buf.at[1], w1_ref)
        waits += keep(1, u, hidden, a2)
        settle(sent_3 + sent_4)
        return moved, waits

    def exchange(half, buf, stage, u, hidden, a2):
        sent = []

        def to_peers(kind, pick, dst):
            for o in range(1, dpn):
                copy = send(
                    pick(dp_dest(o)), dst, sem_ds.at[half, kind, o - 1], sem_dr.at[half, kind, o - 1],
                    "dp", dp_dest(o),
                )
                copy.start()
                sent.append(copy)

        if stage == 0:
            rows_all[half, dpi] = u
            hid_all[half, dpi] = hidden
            to_peers(0, lambda d: rows_all.at[half, dpi], rows_all.at[half, dpi])
            to_peers(1, lambda d: hid_all.at[half, dpi], hid_all.at[half, dpi])
        g = 0 if stage == 0 else 1
        for k in range(q):
            g_all[half, g, k, dpi] = buf[g, dpi * q + k]
            to_peers(2 + g * q + k, lambda d, k=k: buf.at[g, d * q + k], g_all.at[half, g, k, dpi])
        if stage == 0:
            energy = folded(read_ref[...] * (a2 * jax.nn.sigmoid(a2)))
            own_stat[0] = energy if half == 0 else own_stat[0] - energy
        return sent

    def nothing(stage, u, hidden, a2):
        return []

    moved, sent_data = one_pass(data_ref[...], 1.0, ag_data, functools.partial(exchange, 0, ag_data))

    state[...] = start_ref[...]

    def langevin(step, carry):
        moved, _ = one_pass(state[...].astype(BF16), 1.0, ag_neg, nothing)
        state[...] = state[...] - 0.005 * moved + 0.1 * noise_ref[step]
        return carry

    lax.fori_loop(0, steps, langevin, 0)

    moved, sent_neg = one_pass(
        state[...].astype(BF16), -1.0, ag_neg, functools.partial(exchange, 1, ag_neg)
    )

    def arrived(half, kinds):
        for kind in kinds:
            for o in range(1, dpn):
                at = (dpi + dpn - o) % dpn
                if kind == 0:
                    ref = rows_all.at[half, at]
                elif kind == 1:
                    ref = hid_all.at[half, at]
                else:
                    ref = g_all.at[half, (kind - 2) // q, (kind - 2) % q, at]
                send(
                    ref, ref, sem_ds.at[half, kind, o - 1], sem_dr.at[half, kind, o - 1],
                    "dp", dp_dest(o),
                ).wait_recv()

    for half in range(2):
        arrived(half, range(2 + 2 * q))

    def contract(left, right):
        return lax.dot_general(
            left.reshape(-1, left.shape[-1]), right.reshape(-1, right.shape[-1]),
            (((0,), (0,)), ((), ())), preferred_element_type=F32,
        )

    squares = jnp.zeros((8, 128), F32)
    for g, left, out_ref in ((1, rows_all, raw1_ref), (0, hid_all, raw2_ref)):
        for k in range(q):
            raw = contract(left[0], g_all[0, g, k]) + contract(left[1], g_all[1, g, k])
            out_ref[:, k * C : (k + 1) * C] = raw
            squares += folded(raw * raw)
    own_stat[1] = squares

    settle(sent_data + sent_neg)

    base = 0
    for axis, count, peer in (
        ("fsdp", X, lambda o: dest(0, o)), ("fsdp", Z, lambda o: dest(o, 0)), ("dp", dpn, dp_dest),
    ):
        copies = []
        for o in range(1, count):
            at = base + o - 1
            copy = send(own_stat, got_stat.at[at], sem_ts.at[at], sem_tr.at[at], axis, peer(o))
            copy.start()
            copies.append(copy)
        total = own_stat[...]
        for o, copy in enumerate(copies):
            copy.wait()
            total += got_stat[base + o]
        own_stat[...] = total
        base += count - 1
    stat_ref[...] = own_stat[...]


def solution(mesh):
    n, dpn = mesh.shape["fsdp"], mesh.shape["dp"]
    X = inner_of(n)
    Z = n // X
    q = n // dpn

    def local(data, start, noise, w1, w2, readout):
        R, K = start.shape
        H = w1.shape[1]
        C = H // n
        steps = noise.shape[0]
        vmem = pl.BlockSpec(memory_space=pltpu.VMEM)
        dma = pltpu.SemaphoreType.DMA
        kinds = 2 + 2 * q
        peers = (X - 1) + (Z - 1) + (dpn - 1)
        raw1, raw2, stat = pl.pallas_call(
            functools.partial(kernel, n, X, dpn, steps),
            name="contrastive",
            out_shape=(
                jax.ShapeDtypeStruct((K, q * C), F32),
                jax.ShapeDtypeStruct((C, q * C), F32),
                jax.ShapeDtypeStruct((2, 8, 128), F32),
            ),
            in_specs=[vmem] * 6,
            out_specs=(vmem,) * 3,
            scratch_shapes=[
                pltpu.VMEM((R, K), F32),
                pltpu.VMEM((2, Z, X - 1, R, C), BF16),
                pltpu.VMEM((2, Z, X - 1, R, C), BF16),
                pltpu.VMEM((2, Z - 1, R, C), BF16),
                pltpu.VMEM((2, Z - 1, R, C), BF16),
                pltpu.VMEM((Z, R, C), F32),
                pltpu.VMEM((2, n, R, C), BF16),
                pltpu.VMEM((2, n, R, C), BF16),
                pltpu.VMEM((2, dpn, R, K), BF16),
                pltpu.VMEM((2, dpn, R, C), BF16),
                pltpu.VMEM((2, 2, q, dpn, R, C), BF16),
                pltpu.VMEM((2, 8, 128), F32),
                pltpu.VMEM((peers, 2, 8, 128), F32),
                dma((2, Z, X - 1)), dma((2, Z, X - 1)),
                dma((2, Z - 1)), dma((2, Z - 1)),
                dma((2, Z - 1)), dma((2, Z - 1)),
                dma((2, Z, X - 1)), dma((2, Z, X - 1)),
                dma((2, kinds, dpn - 1)), dma((2, kinds, dpn - 1)),
                dma((peers,)), dma((peers,)),
            ],
            compiler_params=pltpu.CompilerParams(
                collective_id=0, has_side_effects=True, vmem_limit_bytes=60 * 1024 * 1024
            ),
        )(data, start, noise, w1, w2, readout.reshape(1, C))
        sums = jnp.sum(stat, axis=(1, 2))
        energy_gap = sums[0] / (R * dpn * 80.0 * jnp.sqrt(jnp.float32(H)))
        scale = jnp.sqrt(sums[1] / (2.0 * (K * n) * H) + 1e-06)
        return raw1 / scale, raw2 / scale, energy_gap

    in_specs = (
        P("dp", "fsdp"),
        P("dp", "fsdp"),
        P(None, "dp", "fsdp"),
        P("fsdp", None),
        P("fsdp", None),
        P("fsdp"),
    )
    out_specs = (P("fsdp", "dp"), P("fsdp", "dp"), P())
    return jax.shard_map(local, mesh=mesh, in_specs=in_specs, out_specs=out_specs, check_vma=False)
```

```python
import functools

import jax
import jax.numpy as jnp
from jax import lax
from jax.experimental import pallas as pl
from jax.experimental.pallas import tpu as pltpu
from jax.sharding import PartitionSpec as P

MESH = pl.DeviceIdType.MESH
BF16 = jnp.bfloat16
F32 = jnp.float32


def inner_of(n):
    return max(i for i in range(1, n + 1) if n % i == 0 and i * i <= n)


def folded(values):
    rows, columns = values.shape
    tall = values.reshape(rows // 8, 8, columns).sum(axis=0)
    out = tall[:, :128]
    for at in range(128, columns, 128):
        out += tall[:, at : at + 128]
    return out


def kernel(
    n, X, dpn, steps, S,
    data_ref, start_ref, noise_ref, w1_ref, w2_ref, read_ref,
    raw1_ref, raw2_ref, stat_ref,
    state, s_a, r_a, s_b, r_b, acc, ag_data, ag_neg, rows_all, hid_all, g_all, own_stat, got_stat,
    sem_as, sem_ar, sem_bs, sem_br, sem_zs, sem_zr, sem_xs, sem_xr, sem_ds, sem_dr, sem_ts, sem_tr,
):
    Z = n // X
    q = n // dpn
    C = w1_ref.shape[1] // n
    height = data_ref.shape[0] // S
    me = lax.axis_index("fsdp")
    dpi = lax.axis_index("dp")
    z, x = me // X, me % X

    def dest(oz, ox):
        return ((z + oz) % Z) * X + (x + ox) % X

    def source(oz, ox):
        return ((z + Z - oz) % Z) * X + (x + X - ox) % X

    def dp_dest(o):
        return (dpi + o) % dpn

    def cols(at):
        return pl.ds(pl.multiple_of(at * C, C), C)

    def send(src, dst, ssem, rsem, axis, peer):
        return pltpu.make_async_remote_copy(
            src_ref=src, dst_ref=dst, send_sem=ssem, recv_sem=rsem,
            device_id={axis: peer}, device_id_type=MESH,
        )

    partners = (
        [("fsdp", dest(0, ox)) for ox in range(1, X)]
        + [("fsdp", dest(oz, 0)) for oz in range(1, Z)]
        + [("dp", dp_dest(o)) for o in range(1, dpn)]
    )
    barrier = pltpu.get_barrier_semaphore()
    for axis, peer in partners:
        pl.semaphore_signal(barrier, inc=1, device_id={axis: peer}, device_id_type=MESH)
    pl.semaphore_wait(barrier, len(partners))

    def a_copy(s, j, oz, ox):
        return send(
            s_a.at[s, j, oz, ox - 1], r_a.at[s, j, oz, ox - 1],
            sem_as.at[s, j, oz, ox - 1], sem_ar.at[s, j, oz, ox - 1], "fsdp", dest(0, ox),
        )

    def b_copy(s, j, oz):
        return send(
            s_b.at[s, j, oz - 1], r_b.at[s, j, oz - 1],
            sem_bs.at[s, j, oz - 1], sem_br.at[s, j, oz - 1], "fsdp", dest(oz, 0),
        )

    def z_copy(s, j, oz, buf, at):
        ref = buf.at[s, j, at]
        return send(ref, ref, sem_zs.at[s, j, oz - 1], sem_zr.at[s, j, oz - 1], "fsdp", dest(oz, 0))

    def x_copy(s, j, oz, ox, buf, at):
        ref = buf.at[s, j, at]
        return send(
            ref, ref, sem_xs.at[s, j, oz, ox - 1], sem_xr.at[s, j, oz, ox - 1], "fsdp", dest(0, ox)
        )

    def scatter_open(s, j, lhs, w_ref):
        order = list(range(1, Z)) + [0]
        for oz in order:
            for ox in range(1, X):
                s_a[s, j, oz, ox - 1] = jnp.dot(
                    lhs, w_ref[:, cols(dest(oz, ox))], preferred_element_type=F32
                ).astype(BF16)
                a_copy(s, j, oz, ox).start()
        for oz in order:
            acc[s, oz] = jnp.dot(lhs, w_ref[:, cols(dest(oz, 0))], preferred_element_type=F32)

    def joined(s, j, oz):
        total = acc[s, oz]
        for ox in range(1, X):
            a_copy(s, j, oz, ox).wait_recv()
            total += r_a[s, j, oz, ox - 1].astype(F32)
        return total

    def scatter_join(s, j):
        for oz in range(1, Z):
            s_b[s, j, oz - 1] = joined(s, j, oz).astype(BF16)
            b_copy(s, j, oz).start()

    def scatter_close(s, j):
        total = joined(s, j, 0)
        for oz in range(1, Z):
            b_copy(s, j, oz).wait_recv()
            total += r_b[s, j, oz - 1].astype(F32)
        return total

    def scatter_settle(s, j):
        for oz in range(Z):
            for ox in range(1, X):
                a_copy(s, j, oz, ox).wait_send()
        for oz in range(1, Z):
            b_copy(s, j, oz).wait_send()

    def gather_open(s, j, buf):
        for oz in range(1, Z):
            z_copy(s, j, oz, buf, me).start()
        for ox in range(1, X):
            x_copy(s, j, 0, ox, buf, me).start()

    def block(s, j, buf, at, w_ref):
        return lax.dot_general(
            buf[s, j, at], w_ref[:, cols(at)], (((1,), (1,)), ((), ())), preferred_element_type=F32
        )

    def gather_forward(s, j, buf, w_ref):
        total = None if w_ref is None else block(s, j, buf, me, w_ref)
        for oz in range(1, Z):
            at = source(oz, 0)
            z_copy(s, j, oz, buf, at).wait_recv()
            for ox in range(1, X):
                x_copy(s, j, oz, ox, buf, at).start()
            if w_ref is not None:
                total += block(s, j, buf, at, w_ref)
        return total

    def gather_close(s, j, buf, w_ref, total):
        for oz in range(Z):
            for ox in range(1, X):
                at = source(oz, ox)
                x_copy(s, j, oz, ox, buf, at).wait_recv()
                if w_ref is not None:
                    total += block(s, j, buf, at, w_ref)
        return total

    def gather_settle(s, j, buf):
        for oz in range(1, Z):
            z_copy(s, j, oz, buf, me).wait_send()
        for oz in range(Z):
            for ox in range(1, X):
                x_copy(s, j, oz, ox, buf, source(oz, 0)).wait_send()

    def stages(s, u, sign, buf, keep, after, w_back):
        scatter_join(s, 0)
        yield
        a1 = scatter_close(s, 0)
        s1 = jax.nn.sigmoid(a1)
        hidden = (a1 * s1).astype(BF16)
        slope_1 = s1 * (1.0 + a1 * (1.0 - s1))
        scatter_open(s, 1, hidden, w2_ref)
        scatter_settle(s, 0)
        yield
        scatter_join(s, 1)
        yield
        a2 = scatter_close(s, 1)
        s2 = jax.nn.sigmoid(a2)
        buf[s, 0, me] = (sign * read_ref[...] * (s2 * (1.0 + a2 * (1.0 - s2)))).astype(BF16)
        gather_open(s, 0, buf)
        scatter_settle(s, 1)
        yield
        total = gather_forward(s, 0, buf, w2_ref)
        yield
        back = gather_close(s, 0, buf, w2_ref, total)
        buf[s, 1, me] = (back * slope_1).astype(BF16)
        gather_open(s, 1, buf)
        keep(s, 0, u, hidden, a2 * s2)
        yield
        total = gather_forward(s, 1, buf, w_back)
        yield
        moved = gather_close(s, 1, buf, w_back, total)
        keep(s, 1, u, hidden, None)
        gather_settle(s, 0, buf)
        gather_settle(s, 1, buf)
        after(s, moved)

    def interleave(passes):
        passes = list(passes)
        while passes:
            passes = [p for p in passes if next(p, passes) is not passes]

    def dp_ref(half, kind, d, s):
        if kind == 0:
            return rows_all.at[half, d, s]
        if kind == 1:
            return hid_all.at[half, d, s]
        return g_all.at[half, (kind - 2) // q, (kind - 2) % q, d, s]

    def dp_copy(half, kind, o, s, src, d):
        return send(
            src, dp_ref(half, kind, d, s), sem_ds.at[half, kind, o - 1, s],
            sem_dr.at[half, kind, o - 1, s], "dp", dp_dest(o),
        )

    def dp_copies(half, buf, s, stage):
        kinds = ([0, 1] if stage == 0 else []) + [2 + stage * q + k for k in range(q)]
        for kind in kinds:
            for o in range(1, dpn):
                if kind < 2:
                    own = dp_ref(half, kind, dpi, s)
                else:
                    own = buf.at[s, stage, dp_dest(o) * q + (kind - 2) % q]
                yield dp_copy(half, kind, o, s, own, dpi)

    def exchange(half, buf, s, stage, u, hidden, silu_2):
        if stage == 0:
            rows_all[half, dpi, s] = u
            hid_all[half, dpi, s] = hidden
            energy = folded(read_ref[...] * silu_2)
            if half == 0 and s == 0:
                own_stat[0] = energy
            else:
                own_stat[0] = own_stat[0] + energy if half == 0 else own_stat[0] - energy
        for k in range(q):
            g_all[half, stage, k, dpi, s] = buf[s, stage, dpi * q + k]
        for copy in dp_copies(half, buf, s, stage):
            copy.start()

    def nothing(*args):
        return None

    def rows_of(s):
        return pl.ds(s * height, height)

    def opened(s, *args):
        scatter_open(s, 0, state[rows_of(s), :].astype(BF16), w1_ref)

    streams = range(S)
    for s in streams:
        scatter_open(s, 0, data_ref[rows_of(s), :], w1_ref)
    state[...] = start_ref[...]
    interleave(
        stages(
            s, data_ref[rows_of(s), :], 1.0, ag_data, functools.partial(exchange, 0, ag_data), opened, None
        )
        for s in streams
    )

    def langevin(step, carry):
        def after(s, moved):
            at = rows_of(s)
            state[at, :] = state[at, :] - 0.005 * moved + 0.1 * noise_ref[step, at, :]
            opened(s)

        interleave(stages(s, None, 1.0, ag_neg, nothing, after, w1_ref) for s in streams)
        return carry

    lax.fori_loop(0, steps, langevin, 0)

    def contract(left, right):
        return lax.dot_general(
            left.reshape(-1, left.shape[-1]), right.reshape(-1, right.shape[-1]),
            (((0,), (0,)), ((), ())), preferred_element_type=F32,
        )

    def arrived(half, kinds):
        for s in streams:
            for kind in kinds:
                for o in range(1, dpn):
                    at = (dpi + dpn - o) % dpn
                    dp_copy(half, kind, o, s, dp_ref(half, kind, at, s), at).wait_recv()

    def gradients():
        for _ in range(6):
            yield
        arrived(0, range(2 + 2 * q))
        for g, left, out_ref in ((1, rows_all, raw1_ref), (0, hid_all, raw2_ref)):
            for k in range(q):
                out_ref[:, k * C : (k + 1) * C] = contract(left[0], g_all[0, g, k])

    interleave(
        [
            stages(
                s, state[rows_of(s), :].astype(BF16), -1.0, ag_neg,
                functools.partial(exchange, 1, ag_neg), nothing, None,
            )
            for s in streams
        ]
        + [gradients()]
    )

    squares = jnp.zeros((8, 128), F32)
    for g, left, out_ref in ((0, hid_all, raw2_ref), (1, rows_all, raw1_ref)):
        arrived(1, ([0, 1] if g == 0 else []) + [2 + g * q + k for k in range(q)])
        for k in range(q):
            at = slice(k * C, (k + 1) * C)
            raw = out_ref[:, at] + contract(left[1], g_all[1, g, k])
            out_ref[:, at] = raw
            squares += folded(raw * raw)
    own_stat[1] = squares

    for half, buf in ((0, ag_data), (1, ag_neg)):
        for s in streams:
            for stage in range(2):
                for copy in dp_copies(half, buf, s, stage):
                    copy.wait_send()

    base = 0
    for axis, count, peer in (
        ("fsdp", X, lambda o: dest(0, o)), ("fsdp", Z, lambda o: dest(o, 0)), ("dp", dpn, dp_dest),
    ):
        copies = []
        for o in range(1, count):
            at = base + o - 1
            copy = send(own_stat, got_stat.at[at], sem_ts.at[at], sem_tr.at[at], axis, peer(o))
            copy.start()
            copies.append(copy)
        total = own_stat[...]
        for o, copy in enumerate(copies):
            copy.wait()
            total += got_stat[base + o]
        own_stat[...] = total
        base += count - 1
    stat_ref[...] = own_stat[...]


def solution(mesh):
    n, dpn = mesh.shape["fsdp"], mesh.shape["dp"]
    X = inner_of(n)
    Z = n // X
    q = n // dpn

    def local(data, start, noise, w1, w2, readout):
        R, K = start.shape
        H = w1.shape[1]
        C = H // n
        steps = noise.shape[0]
        S = 2 if R % 32 == 0 else 1
        h = R // S
        vmem = pl.BlockSpec(memory_space=pltpu.VMEM)
        dma = pltpu.SemaphoreType.DMA
        kinds = 2 + 2 * q
        peers = (X - 1) + (Z - 1) + (dpn - 1)
        raw1, raw2, stat = pl.pallas_call(
            functools.partial(kernel, n, X, dpn, steps, S),
            name="contrastive",
            out_shape=(
                jax.ShapeDtypeStruct((K, q * C), F32),
                jax.ShapeDtypeStruct((C, q * C), F32),
                jax.ShapeDtypeStruct((2, 8, 128), F32),
            ),
            in_specs=[vmem] * 6,
            out_specs=(vmem,) * 3,
            scratch_shapes=[
                pltpu.VMEM((R, K), F32),
                pltpu.VMEM((S, 2, Z, X - 1, h, C), BF16),
                pltpu.VMEM((S, 2, Z, X - 1, h, C), BF16),
                pltpu.VMEM((S, 2, Z - 1, h, C), BF16),
                pltpu.VMEM((S, 2, Z - 1, h, C), BF16),
                pltpu.VMEM((S, Z, h, C), F32),
                pltpu.VMEM((S, 2, n, h, C), BF16),
                pltpu.VMEM((S, 2, n, h, C), BF16),
                pltpu.VMEM((2, dpn, S, h, K), BF16),
                pltpu.VMEM((2, dpn, S, h, C), BF16),
                pltpu.VMEM((2, 2, q, dpn, S, h, C), BF16),
                pltpu.VMEM((2, 8, 128), F32),
                pltpu.VMEM((peers, 2, 8, 128), F32),
                dma((S, 2, Z, X - 1)), dma((S, 2, Z, X - 1)),
                dma((S, 2, Z - 1)), dma((S, 2, Z - 1)),
                dma((S, 2, Z - 1)), dma((S, 2, Z - 1)),
                dma((S, 2, Z, X - 1)), dma((S, 2, Z, X - 1)),
                dma((2, kinds, dpn - 1, S)), dma((2, kinds, dpn - 1, S)),
                dma((peers,)), dma((peers,)),
            ],
            compiler_params=pltpu.CompilerParams(
                collective_id=0, has_side_effects=True, vmem_limit_bytes=60 * 1024 * 1024
            ),
        )(data, start, noise, w1, w2, readout.reshape(1, C))
        sums = jnp.sum(stat, axis=(1, 2))
        energy_gap = sums[0] / (R * dpn * 80.0 * jnp.sqrt(jnp.float32(H)))
        scale = jnp.sqrt(sums[1] / (2.0 * (K * n) * H) + 1e-06)
        return raw1 / scale, raw2 / scale, energy_gap

    in_specs = (
        P("dp", "fsdp"),
        P("dp", "fsdp"),
        P(None, "dp", "fsdp"),
        P("fsdp", None),
        P("fsdp", None),
        P("fsdp"),
    )
    out_specs = (P("fsdp", "dp"), P("fsdp", "dp"), P())
    return jax.shard_map(local, mesh=mesh, in_specs=in_specs, out_specs=out_specs, check_vma=False)
```
